32 devices in a mesh: gx: 4 (over z), gy: 4 (over y, core), gz: 2 (over x).
Axes of the slice: x: 2, y: 2, z: 4, core: 2. Of those that a mesh axis runs over, the one named last changes fastest.
Arguments:
- right_side: float32 [128, 128, 256], P('gx', 'gy', 'gz'), may hold values from -8 to 8
- guess: float32 [128, 128, 256], P('gx', 'gy', 'gz'), may hold values from -4 to 4
Outputs:
- solution_field: float32 [128, 128, 256], P('gx', 'gy', 'gz')
- residual: float32 [128, 128, 256], P('gx', 'gy', 'gz')
The draws below stay inside these ranges and needn't reach their ends.
All inputs are finite; a program needn't handle non-finite values.
Results may differ from the reference program's by a relative error of at most 0.0001.
Values sent between devices are 32-bit elements; how exact they have to be, the bound alone decides.
A program may use at most 128 MiB of HBM per device.

```python
import jax
import jax.numpy as jnp

LEVELS = 6
SWEEPS = 4
STEPS = 2
NX = 128
NY = 128
NZ = 256


def level_of(stream_key, dims, cuts, low, largest):
    level = 1.0
    for position, shards_of in cuts:
        heights = jax.random.uniform(jax.random.fold_in(jax.random.fold_in(stream_key, 6), position), (shards_of,), jnp.float32, low / len(cuts), largest / len(cuts))
        level = level * jnp.repeat(jnp.exp(heights), dims[position] // shards_of).reshape((-1,) + (1,) * (len(dims) - 1 - position))
    return level


def centred(own_key, shape, width, limit, pieces=(), kind=jnp.bfloat16):
    drawn = width * jax.random.normal(own_key, shape, jnp.float32)
    if pieces:
        drawn = drawn * level_of(own_key, shape, pieces, -0.22, 0.18)
    return jnp.clip(drawn, -limit, limit).astype(kind)


def setup_inputs(seed: int = 0) -> dict:
    keys = jax.random.split(jax.random.key(seed), 3)
    return {
        "right_side": centred(keys[0], (NX, NY, NZ), 1.0, 8.0, ((0, 4), (1, 4), (2, 2)), jnp.float32),
        "guess": centred(keys[1], (NX, NY, NZ), 0.5, 4.0, ((0, 4), (1, 4), (2, 2)), jnp.float32),
    }


damping = 2.0 / 3.0


def stencil(field):
    padded = jnp.pad(field, 1)
    beside = padded[2:, 1:-1, 1:-1] + padded[:-2, 1:-1, 1:-1]
    beside = beside + padded[1:-1, 2:, 1:-1] + padded[1:-1, :-2, 1:-1]
    beside = beside + padded[1:-1, 1:-1, 2:] + padded[1:-1, 1:-1, :-2]
    return 6.0 * field - beside


def restrict(field):
    first, second, third = field.shape
    blocks = field.reshape(first // 2, 2, second // 2, 2, third // 2, 2)
    return jnp.mean(blocks, axis=(1, 3, 5))


def prolong(field):
    first, second, third = field.shape
    spread = jnp.broadcast_to(field[:, None, :, None, :, None], (first, 2, second, 2, third, 2))
    return spread.reshape(first * 2, second * 2, third * 2)


def smooth(rhs, level_index):
    scaling = 0.25 ** level_index
    diagonal_value = 6.0 * scaling
    approx = damping * rhs / diagonal_value
    for sweep_index in range(SWEEPS - 1):
        approx = approx + damping * (rhs - scaling * stencil(approx)) / diagonal_value
    return approx


def precondition(residual):
    chain = [residual]
    for level_index in range(1, LEVELS):
        chain.append(restrict(chain[-1]))
    correction = smooth(chain[LEVELS - 1], LEVELS - 1)
    for level_index in range(LEVELS - 2, -1, -1):
        correction = prolong(correction) + smooth(chain[level_index], level_index)
    return correction


def reference(right_side, guess):
    solution_field = guess
    residual = right_side - stencil(guess)
    for step_index in range(STEPS):
        direction = precondition(residual)
        image = stencil(direction)
        alpha = jnp.sum(residual * direction) / jnp.sum(direction * image)
        solution_field = solution_field + alpha * direction
        residual = residual - alpha * image
    return solution_field, residual
```

```python
import functools

import jax
import jax.numpy as jnp
from jax import lax
from jax.experimental import pallas as pl
from jax.experimental.pallas import tpu as pltpu
from jax.sharding import PartitionSpec as P

LEVELS = 6
SWEEPS = 4
STEPS = 2
HALOED = 3
AXES = ("gx", "gy", "gz")
LANES = 128
TOP = 8
MESH = pl.DeviceIdType.MESH
ROUNDS = 1 + STEPS * SWEEPS
HIGH = lax.Precision.HIGHEST


def iota(shape, dim):
    return lax.broadcasted_iota(jnp.int32, shape, dim)


def lanes_dot(x, matrix):
    first, second, _ = x.shape
    if second % 8 == 0:
        out = jnp.dot(x.reshape(first * second, LANES), matrix, precision=HIGH, preferred_element_type=jnp.float32)
        return out.reshape(first, second, LANES)
    planes = [jnp.dot(x[i], matrix, precision=HIGH, preferred_element_type=jnp.float32)[None] for i in range(first)]
    return jnp.concatenate(planes, axis=0)


def halve_matrix(width, start):
    source, target = iota((LANES, LANES), 0), iota((LANES, LANES), 1) - start
    keep = (target >= 0) & (target < width) & ((source == 2 * target) | (source == 2 * target + 1))
    return jnp.where(keep, 0.125, 0.0)


def double_matrix(width, start):
    source, target = iota((LANES, LANES), 0) - start, iota((LANES, LANES), 1)
    keep = (source >= 0) & (source < width) & ((target == 2 * source) | (target == 2 * source + 1))
    return jnp.where(keep, 1.0, 0.0)


def kernel(sizes, block, b_ref, x_ref, sol_ref, res_ref, *rest):
    (u0a, u0b, u1a, u1b, u2a, u2b, g0, g1, g2, wref, fold, spread,
     xs, xr, ys, yr, zs, zr, gs, gr, ds, dr,
     hsend, hrecv, gsend, grecv, dsend, drecv) = rest
    us = ((u0a, u0b), (u1a, u1b), (u2a, u2b))
    gref = (g0, g1, g2)
    nx, ny, nz = sizes
    n = nx * ny * nz
    at = tuple(lax.axis_index(a) for a in AXES)
    me = (at[0] * ny + at[1]) * nz + at[2]
    dims = [tuple(d >> l for d in block) for l in range(LEVELS)]

    def place(index):
        return (index // (ny * nz), index // nz % ny, index % nz)

    xr[...] = jnp.zeros_like(xr)
    yr[...] = jnp.zeros_like(yr)
    zr[...] = jnp.zeros_like(zr)

    barrier = pltpu.get_barrier_semaphore()

    def greet(k, _):
        pl.semaphore_signal(barrier, inc=1, device_id=place((me + k) % n), device_id_type=MESH)
        return 0

    lax.fori_loop(1, n, greet, 0)
    pl.semaphore_wait(barrier, n - 1)

    row_off, lane_off = [0], [0]
    for l in range(HALOED):
        row_off.append(row_off[-1] + dims[l][0])
        lane_off.append(lane_off[-1] + 2 * dims[l][0])

    def halo_copies(r, levels):
        rows = row_off[levels]
        out = []
        for d, (s, t) in enumerate(((xs, xr), (ys, yr), (zs, zr))):
            for side in (0, 1):
                target = list(at)
                target[d] = at[d] + (1 if side else -1)
                src = s.at[r] if d == 2 else s.at[r, side, pl.ds(0, rows)]
                dst = t.at[r, side] if d == 2 else t.at[r, side, pl.ds(0, rows)]
                copy = pltpu.make_async_remote_copy(
                    src_ref=src, dst_ref=dst,
                    send_sem=hsend.at[r, 2 * d + side], recv_sem=hrecv.at[r, 2 * d + side],
                    device_id=tuple(target), device_id_type=MESH,
                )
                lower, upper = at[d] > 0, at[d] < sizes[d] - 1
                out.append((copy, upper if side else lower, lower if side else upper))
        return out

    def send(r, fields, levels):
        for l in range(levels):
            X, Y, Z = dims[l]
            u = fields[l]
            o = row_off[l]
            for side, i in ((0, 1), (1, X)):
                xs[r, side, o:o + Y, :] = u[i, TOP:TOP + Y, :]
            for side, j in ((0, TOP), (1, TOP + Y - 1)):
                ys[r, side, o:o + X, :, :] = u[1:X + 1, j:j + 1, :]
            body = u[1:X + 1, TOP:TOP + Y, :]
            lane, plane = iota((X, Y, LANES), 2) - lane_off[l], iota((X, Y, LANES), 0)
            packed = jnp.where(lane == plane, body[:, :, Z - 1:Z], jnp.where(lane == plane + X, body[:, :, 0:1], 0.0))
            packed = jnp.sum(packed, axis=0)
            zs[r, 0:Y, :] = packed if l == 0 else zs[r, 0:Y, :] + packed
        for copy, cond, _ in halo_copies(r, levels):
            pl.when(cond)(copy.start)

    def receive(r, fields, levels):
        for copy, _, cond in halo_copies(r, levels):
            pl.when(cond)(copy.wait_recv)
        for l in range(levels):
            X, Y, Z = dims[l]
            u = fields[l]
            o = row_off[l]
            u[0, TOP:TOP + Y, :] = xr[r, 1, o:o + Y, :]
            u[X + 1, TOP:TOP + Y, :] = xr[r, 0, o:o + Y, :]
            u[1:X + 1, TOP - 1:TOP, :] = yr[r, 1, o:o + X, :, :]
            u[1:X + 1, TOP + Y:TOP + Y + 1, :] = yr[r, 0, o:o + X, :, :]

    def beside(r, u, l, x0, c):
        X, Y, Z = dims[l]
        mid = u[x0 + 1:x0 + 1 + c, TOP:TOP + Y, :]
        total = u[x0:x0 + c, TOP:TOP + Y, :] + u[x0 + 2:x0 + 2 + c, TOP:TOP + Y, :]
        total = total + u[x0 + 1:x0 + 1 + c, TOP - 1:TOP - 1 + Y, :]
        total = total + u[x0 + 1:x0 + 1 + c, TOP + 1:TOP + 1 + Y, :]
        lane = iota((c, Y, LANES), 2)
        o = lane_off[l] + x0
        low, high = zr[r, 1, 0:Y, :], zr[r, 0, 0:Y, :]
        below = jnp.concatenate([low[:, o + i:o + i + 1][None] for i in range(c)], axis=0)
        above = jnp.concatenate([high[:, o + X + i:o + X + i + 1][None] for i in range(c)], axis=0)
        total = total + jnp.where(lane == 0, below, pltpu.roll(mid, 1, 2))
        total = total + jnp.where(lane == Z - 1, above, pltpu.roll(mid, LANES - 1, 2))
        return mid, total

    def chunks(l):
        c = min(dims[l][0], 4)
        return [(x0, c) for x0 in range(0, dims[l][0], c)]

    def inside(l, x0, c):
        return (slice(x0 + 1, x0 + 1 + c), slice(TOP, TOP + dims[l][1]), slice(None))

    def fold_xy(field):
        X, Y, _ = field.shape
        pairs = field.reshape(X // 2, 2, Y, LANES)
        fold[0:X // 2, 0:Y, :] = pairs[:, 0] + pairs[:, 1]
        return fold[0:X // 2, pl.ds(0, Y // 2, 2), :] + fold[0:X // 2, pl.ds(1, Y // 2, 2), :]

    def spread_y(field):
        X, Y, _ = field.shape
        spread[0:X, pl.ds(0, Y, 2), :] = field
        spread[0:X, pl.ds(1, Y, 2), :] = field

    def twice(field):
        X, Y, _ = field.shape
        return jnp.broadcast_to(field[:, None], (X, 2, Y, LANES)).reshape(2 * X, Y, LANES)

    def all_copy(k, src, dst, s_sem, r_sem):
        return pltpu.make_async_remote_copy(
            src_ref=src, dst_ref=dst.at[me], send_sem=s_sem.at[k], recv_sem=r_sem.at[k],
            device_id=place((me + k) % n), device_id_type=MESH,
        )

    def to_all(step, src, dst, s_sem, r_sem, what):
        def one(k, _):
            copy = all_copy(k, src.at[step], dst.at[step], s_sem.at[step], r_sem.at[step])
            getattr(copy, what)()
            return 0
        lax.fori_loop(1, n, one, 0)

    X, Y, Z = dims[0]
    u0a[1:X + 1, TOP:TOP + Y, :] = x_ref[...]
    sol_ref[...] = x_ref[...]
    send(0, [u0a], 1)
    receive(0, [u0a], 1)
    for x0, c in chunks(0):
        mid, total = beside(0, u0a, 0, x0, c)
        g0[x0:x0 + c] = b_ref[x0:x0 + c] - (6.0 * mid - total)

    def smooth_whole(rhs, width, l):
        X, Y, _ = rhs.shape
        lane = iota(rhs.shape, 2)
        e = rhs
        for _ in range(SWEEPS - 1):
            px, py = jnp.zeros((1, Y, LANES), jnp.float32), jnp.zeros((X, 1, LANES), jnp.float32)
            total = jnp.concatenate([px, e[:-1]], axis=0) + jnp.concatenate([e[1:], px], axis=0)
            total = total + jnp.concatenate([py, e[:, :-1]], axis=1) + jnp.concatenate([e[:, 1:], py], axis=1)
            total = total + jnp.where(lane == 0, 0.0, pltpu.roll(e, 1, 2))
            total = total + jnp.where(lane == width - 1, 0.0, pltpu.roll(e, LANES - 1, 2))
            e = rhs + (3.0 * e + total) * (1.0 / 9.0)
        return e * (4.0 ** l / 9.0)

    for step in range(STEPS):
        base = 1 + step * SWEEPS
        for l in range(HALOED - 1):
            gref[l + 1][...] = lanes_dot(fold_xy(gref[l][...]), halve_matrix(dims[l + 1][2], 0))
        width = dims[HALOED][2]
        own = lanes_dot(fold_xy(gref[HALOED - 1][...]), halve_matrix(width, at[2] * width))
        gs[step] = own
        gr[step, me] = own
        to_all(step, gs, gr, gsend, grecv, "start")
        for l in range(HALOED):
            us[l][0][1:dims[l][0] + 1, TOP:TOP + dims[l][1], :] = gref[l][...]
        for sweep in range(SWEEPS - 1):
            r = base + sweep
            fields = [us[l][sweep % 2] for l in range(HALOED)]
            later = [us[l][(sweep + 1) % 2] for l in range(HALOED)]
            send(r, fields, HALOED)
            if sweep == SWEEPS - 2:
                to_all(step, gs, gr, gsend, grecv, "wait_recv")
                rows = []
                for i in range(nx):
                    columns = []
                    for j in range(ny):
                        part = gr[step, (i * ny + j) * nz]
                        for k in range(1, nz):
                            part = part + gr[step, (i * ny + j) * nz + k]
                        columns.append(part)
                    rows.append(jnp.concatenate(columns, axis=1))
                chain = [jnp.concatenate(rows, axis=0)]
                widths = [width * nz]
                for l in range(HALOED + 1, LEVELS):
                    widths.append(widths[-1] // 2)
                    chain.append(lanes_dot(fold_xy(chain[-1]), halve_matrix(widths[-1], 0)))
                whole = smooth_whole(chain[-1], widths[-1], LEVELS - 1)
                for l in range(LEVELS - 2, HALOED - 1, -1):
                    i = l - HALOED
                    spread_y(whole)
                    grown = spread[0:whole.shape[0], 0:2 * whole.shape[1], :]
                    grown = twice(lanes_dot(grown, double_matrix(widths[i + 1], 0)))
                    whole = grown + smooth_whole(chain[i], widths[i], l)
                wref[...] = whole
            receive(r, fields, HALOED)
            for l in range(HALOED):
                for x0, c in chunks(l):
                    mid, total = beside(r, fields[l], l, x0, c)
                    later[l][inside(l, x0, c)] = gref[l][x0:x0 + c] + (3.0 * mid + total) * (1.0 / 9.0)
        ends = [us[l][(SWEEPS - 1) % 2] for l in range(HALOED)]
        cx, cy, _ = dims[HALOED]
        spread_y(wref[pl.ds(at[0] * cx, cx)])
        part = spread[0:cx, pl.ds(pl.multiple_of(at[1] * 2 * cy, 8), 2 * cy), :]
        part = lanes_dot(part, double_matrix(width, at[2] * width))
        for l in range(HALOED - 1, -1, -1):
            X, Y, Z = dims[l]
            full = ends[l][1:X + 1, TOP:TOP + Y, :] * (4.0 ** l / 9.0) + twice(part)
            if l:
                spread_y(full)
                part = lanes_dot(spread[0:X, 0:2 * Y, :], double_matrix(Z, 0))
            else:
                ends[0][1:X + 1, TOP:TOP + Y, :] = full
        r = base + SWEEPS - 1
        z = ends[0]
        w = us[0][SWEEPS % 2]
        send(r, [z], 1)
        receive(r, [z], 1)
        rz = jnp.zeros((Y, LANES), jnp.float32)
        zw = jnp.zeros((Y, LANES), jnp.float32)
        for x0, c in chunks(0):
            mid, total = beside(r, z, 0, x0, c)
            image = 6.0 * mid - total
            w[inside(0, x0, c)] = image
            rz = rz + jnp.sum(g0[x0:x0 + c] * mid, axis=0)
            zw = zw + jnp.sum(mid * image, axis=0)
        sums = jnp.concatenate([jnp.sum(rz, axis=0, keepdims=True), jnp.sum(zw, axis=0, keepdims=True)], axis=0)
        ds[step] = sums
        dr[step, me] = sums
        to_all(step, ds, dr, dsend, drecv, "start")
        to_all(step, ds, dr, dsend, drecv, "wait_recv")
        both = jnp.sum(dr[step], axis=0)
        both = jnp.sum(both, axis=1, keepdims=True)
        alpha = (both[0:1] / both[1:2])[None]
        for x0, c in chunks(0):
            sol_ref[x0:x0 + c] = sol_ref[x0:x0 + c] + alpha * z[inside(0, x0, c)]
            renewed = g0[x0:x0 + c] - alpha * w[inside(0, x0, c)]
            if step == STEPS - 1:
                res_ref[x0:x0 + c] = renewed
            else:
                g0[x0:x0 + c] = renewed

    for step in range(STEPS):
        to_all(step, gs, gr, gsend, grecv, "wait_send")
        to_all(step, ds, dr, dsend, drecv, "wait_send")
    for r in range(ROUNDS):
        for copy, cond, _ in halo_copies(r, 1 if r % SWEEPS == 0 else HALOED):
            pl.when(cond)(copy.wait_send)


def solution(mesh):
    sizes = tuple(mesh.shape[a] for a in AXES)
    n = sizes[0] * sizes[1] * sizes[2]

    def run(right_side, guess):
        X, Y, Z = block = guess.shape
        dims = [tuple(d >> l for d in block) for l in range(LEVELS)]
        rows = sum(dims[l][0] for l in range(HALOED))
        f32 = jnp.float32
        vm = lambda *s: pltpu.VMEM(s, f32)
        padded = [vm(dims[l][0] + 2, dims[l][1] + 2 * TOP, LANES) for l in range(HALOED) for _ in range(2)]
        cx, cy, _ = dims[HALOED]
        scratch = padded + [vm(dims[l][0], dims[l][1], LANES) for l in range(HALOED)] + [
            vm(cx * sizes[0], cy * sizes[1], LANES),
            vm(X // 2, Y, LANES), vm(X // 2, Y, LANES),
            vm(ROUNDS, 2, rows, LANES), vm(ROUNDS, 2, rows, LANES),
            vm(ROUNDS, 2, rows, 1, LANES), vm(ROUNDS, 2, rows, 1, LANES),
            vm(ROUNDS, Y, LANES), vm(ROUNDS, 2, Y, LANES),
            vm(STEPS, cx, cy, LANES), vm(STEPS, n, cx, cy, LANES),
            vm(STEPS, 2, LANES), vm(STEPS, n, 2, LANES),
            pltpu.SemaphoreType.DMA((ROUNDS, 6)), pltpu.SemaphoreType.DMA((ROUNDS, 6)),
        ] + [pltpu.SemaphoreType.DMA((STEPS, n))] * 4
        out = jax.ShapeDtypeStruct(block, f32)
        return tuple(pl.pallas_call(
            functools.partial(kernel, sizes, block),
            out_shape=(out, out),
            in_specs=[pl.BlockSpec(memory_space=pltpu.VMEM)] * 2,
            out_specs=[pl.BlockSpec(memory_space=pltpu.VMEM)] * 2,
            scratch_shapes=scratch,
            compiler_params=pltpu.CompilerParams(collective_id=0, has_side_effects=True),
        )(right_side, guess))

    spec = P(*AXES)
    return jax.shard_map(run, mesh=mesh, in_specs=(spec, spec), out_specs=(spec, spec), check_vma=False)
```

```python
import functools

import jax
import jax.numpy as jnp
from jax import lax
from jax.experimental import pallas as pl
from jax.experimental.pallas import tpu as pltpu
from jax.sharding import PartitionSpec as P

LEVELS = 6
SWEEPS = 4
STEPS = 2
HALOED = 3
AXES = ("gx", "gy", "gz")
LANES = 128
TOP = 8
MESH = pl.DeviceIdType.MESH
ROUNDS = 1 + STEPS * SWEEPS
HIGH = lax.Precision.HIGHEST


def iota(shape, dim):
    return lax.broadcasted_iota(jnp.int32, shape, dim)


def lanes_dot(x, matrix):
    first, second, _ = x.shape
    if second % 8 == 0:
        out = jnp.dot(x.reshape(first * second, LANES), matrix, precision=HIGH, preferred_element_type=jnp.float32)
        return out.reshape(first, second, LANES)
    planes = [jnp.dot(x[i], matrix, precision=HIGH, preferred_element_type=jnp.float32)[None] for i in range(first)]
    return jnp.concatenate(planes, axis=0)


def halve_matrix(width, start):
    source, target = iota((LANES, LANES), 0), iota((LANES, LANES), 1) - start
    keep = (target >= 0) & (target < width) & ((source == 2 * target) | (source == 2 * target + 1))
    return jnp.where(keep, 0.125, 0.0)


def double_matrix(width, start):
    source, target = iota((LANES, LANES), 0) - start, iota((LANES, LANES), 1)
    keep = (source >= 0) & (source < width) & ((target == 2 * source) | (target == 2 * source + 1))
    return jnp.where(keep, 1.0, 0.0)


def plane_groups(shape, width):
    return max(1, LANES // width // shape[1])


def own_group(shape, width):
    group = iota(shape, 0) % plane_groups(shape, width) * shape[1] + iota(shape, 1)
    return iota(shape, 2) // width == group


def tile_matrix(width):
    source, target = iota((LANES, LANES), 0), iota((LANES, LANES), 1) % width
    return jnp.where((source == 2 * target) | (source == 2 * target + 1), 0.125, 0.0)


def gather_matrix(width, start):
    source, target = iota((LANES, LANES), 0) % width, iota((LANES, LANES), 1) - start
    return jnp.where(source == target, 1.0, 0.0)


def kernel(sizes, block, b_ref, x_ref, sol_ref, res_ref, *rest):
    (u0a, u0b, u1a, u1b, u2a, u2b, g0, g1, g2, wref, fold, spread,
     xs, xr, ys, yr, zs, zr, gs, gr, ds, dr,
     hsend, hrecv, gsend, grecv, dsend, drecv) = rest
    us = ((u0a, u0b), (u1a, u1b), (u2a, u2b))
    gref = (g0, g1, g2)
    nx, ny, nz = sizes
    n = nx * ny * nz
    at = tuple(lax.axis_index(a) for a in AXES)
    me = (at[0] * ny + at[1]) * nz + at[2]
    dims = [tuple(d >> l for d in block) for l in range(LEVELS)]

    def others():
        moved = [[lax.rem(at[d] + k, sizes[d]) if k else at[d] for k in range(sizes[d])] for d in range(3)]
        return [(a, b, c) for a in moved[0] for b in moved[1] for c in moved[2]][1:]

    xr[...] = jnp.zeros_like(xr)
    yr[...] = jnp.zeros_like(yr)
    zr[...] = jnp.zeros_like(zr)

    barrier = pltpu.get_barrier_semaphore()

    for target in others():
        pl.semaphore_signal(barrier, inc=1, device_id=target, device_id_type=MESH)

    row_off, lane_off = [0], [0]
    for l in range(HALOED):
        row_off.append(row_off[-1] + dims[l][0])
        lane_off.append(lane_off[-1] + 2 * dims[l][0])

    def halo_copies(r, levels):
        rows = row_off[levels]
        out = []
        for d, (s, t) in enumerate(((xs, xr), (ys, yr), (zs, zr))):
            for side in (0, 1):
                target = list(at)
                target[d] = at[d] + (1 if side else -1)
                src = s.at[r] if d == 2 else s.at[r, side, pl.ds(0, rows)]
                dst = t.at[r, side] if d == 2 else t.at[r, side, pl.ds(0, rows)]
                copy = pltpu.make_async_remote_copy(
                    src_ref=src, dst_ref=dst,
                    send_sem=hsend.at[r, 2 * d + side], recv_sem=hrecv.at[r, 2 * d + side],
                    device_id=tuple(target), device_id_type=MESH,
                )
                lower, upper = at[d] > 0, at[d] < sizes[d] - 1
                out.append((copy, upper if side else lower, lower if side else upper))
        return out

    def send(r, fields, levels, before=lambda: None):
        for l in range(levels):
            X, Y, Z = dims[l]
            u = fields[l]
            o = row_off[l]
            for side, i in ((0, 1), (1, X)):
                xs[r, side, o:o + Y, :] = u[i, TOP:TOP + Y, :]
            for side, j in ((0, TOP), (1, TOP + Y - 1)):
                ys[r, side, o:o + X, :, :] = u[1:X + 1, j:j + 1, :]
            body = u[1:X + 1, TOP:TOP + Y, :]
            lane, plane = iota((X, Y, LANES), 2) - lane_off[l], iota((X, Y, LANES), 0)
            packed = jnp.where(lane == plane, body[:, :, Z - 1:Z], jnp.where(lane == plane + X, body[:, :, 0:1], 0.0))
            packed = jnp.sum(packed, axis=0)
            zs[r, 0:Y, :] = packed if l == 0 else zs[r, 0:Y, :] + packed
        before()
        for copy, cond, _ in halo_copies(r, levels):
            pl.when(cond)(copy.start)

    def receive(r, fields, levels):
        for copy, _, cond in halo_copies(r, levels):
            pl.when(cond)(copy.wait_recv)
        for l in range(levels):
            X, Y, Z = dims[l]
            u = fields[l]
            o = row_off[l]
            u[0, TOP:TOP + Y, :] = xr[r, 1, o:o + Y, :]
            u[X + 1, TOP:TOP + Y, :] = xr[r, 0, o:o + Y, :]
            u[1:X + 1, TOP - 1:TOP, :] = yr[r, 1, o:o + X, :, :]
            u[1:X + 1, TOP + Y:TOP + Y + 1, :] = yr[r, 0, o:o + X, :, :]

    def beside(r, u, l, x0, c):
        X, Y, Z = dims[l]
        mid = u[x0 + 1:x0 + 1 + c, TOP:TOP + Y, :]
        total = u[x0:x0 + c, TOP:TOP + Y, :] + u[x0 + 2:x0 + 2 + c, TOP:TOP + Y, :]
        total = total + u[x0 + 1:x0 + 1 + c, TOP - 1:TOP - 1 + Y, :]
        total = total + u[x0 + 1:x0 + 1 + c, TOP + 1:TOP + 1 + Y, :]
        lane = iota((c, Y, LANES), 2)
        o = lane_off[l] + x0
        low, high = zr[r, 1, 0:Y, :], zr[r, 0, 0:Y, :]
        below = jnp.concatenate([low[:, o + i:o + i + 1][None] for i in range(c)], axis=0)
        above = jnp.concatenate([high[:, o + X + i:o + X + i + 1][None] for i in range(c)], axis=0)
        total = total + jnp.where(lane == 0, below, pltpu.roll(mid, 1, 2))
        total = total + jnp.where(lane == Z - 1, above, pltpu.roll(mid, LANES - 1, 2))
        return mid, total

    def chunks(l):
        c = min(dims[l][0], 4)
        return [(x0, c) for x0 in range(0, dims[l][0], c)]

    def inside(l, x0, c):
        return (slice(x0 + 1, x0 + 1 + c), slice(TOP, TOP + dims[l][1]), slice(None))

    def fold_xy(field):
        X, Y, _ = field.shape
        pairs = field.reshape(X // 2, 2, Y, LANES)
        fold[0:X // 2, 0:Y, :] = pairs[:, 0] + pairs[:, 1]
        return fold[0:X // 2, pl.ds(0, Y // 2, 2), :] + fold[0:X // 2, pl.ds(1, Y // 2, 2), :]

    def spread_y(field):
        X, Y, _ = field.shape
        spread[0:X, pl.ds(0, Y, 2), :] = field
        spread[0:X, pl.ds(1, Y, 2), :] = field

    def twice(field):
        X, Y, _ = field.shape
        return jnp.broadcast_to(field[:, None], (X, 2, Y, LANES)).reshape(2 * X, Y, LANES)

    def to_all(step, src, dst, s_sem, r_sem):
        for target in others():
            pltpu.make_async_remote_copy(
                src_ref=src.at[step], dst_ref=dst.at[step, me], send_sem=s_sem.at[step], recv_sem=r_sem.at[step],
                device_id=target, device_id_type=MESH,
            ).start()

    def all_done(step, dst, sem):
        part = dst.at[step, pl.ds(0, n - 1)]
        pltpu.make_async_copy(part, part, sem.at[step]).wait()

    X, Y, Z = dims[0]
    u0a[1:X + 1, TOP:TOP + Y, :] = x_ref[...]
    sol_ref[...] = x_ref[...]
    send(0, [u0a], 1, lambda: pl.semaphore_wait(barrier, n - 1))
    receive(0, [u0a], 1)
    for x0, c in chunks(0):
        mid, total = beside(0, u0a, 0, x0, c)
        g0[x0:x0 + c] = b_ref[x0:x0 + c] - (6.0 * mid - total)

    def smooth_whole(rhs, width, l):
        X, Y, _ = rhs.shape
        lane = iota(rhs.shape, 2)
        e = rhs
        for _ in range(SWEEPS - 1):
            px, py = jnp.zeros((1, Y, LANES), jnp.float32), jnp.zeros((X, 1, LANES), jnp.float32)
            total = jnp.concatenate([px, e[:-1]], axis=0) + jnp.concatenate([e[1:], px], axis=0)
            total = total + jnp.concatenate([py, e[:, :-1]], axis=1) + jnp.concatenate([e[:, 1:], py], axis=1)
            total = total + jnp.where(lane == 0, 0.0, pltpu.roll(e, 1, 2))
            total = total + jnp.where(lane == width - 1, 0.0, pltpu.roll(e, LANES - 1, 2))
            e = rhs + (3.0 * e + total) * (1.0 / 9.0)
        return e * (4.0 ** l / 9.0)

    for step in range(STEPS):
        base = 1 + step * SWEEPS
        for l in range(HALOED - 1):
            gref[l + 1][...] = lanes_dot(fold_xy(gref[l][...]), halve_matrix(dims[l + 1][2], 0))
        width = dims[HALOED][2]
        own = lanes_dot(fold_xy(gref[HALOED - 1][...]), tile_matrix(width))
        own = jnp.where(own_group(own.shape, width), own, 0.0)
        own = jnp.sum(own.reshape(-1, plane_groups(own.shape, width), *own.shape[1:]), axis=1)
        own = jnp.sum(own, axis=1, keepdims=True)
        gs[step] = own
        gr[step, me] = own
        to_all(step, gs, gr, gsend, grecv)
        for l in range(HALOED):
            us[l][0][1:dims[l][0] + 1, TOP:TOP + dims[l][1], :] = gref[l][...]
        for sweep in range(SWEEPS - 1):
            r = base + sweep
            fields = [us[l][sweep % 2] for l in range(HALOED)]
            later = [us[l][(sweep + 1) % 2] for l in range(HALOED)]
            send(r, fields, HALOED)
            if sweep == SWEEPS - 2:
                all_done(step, gr, grecv)
                cx, cy, _ = dims[HALOED]
                per = plane_groups((cx, cy), width)
                fine = None
                for k in range(nz):
                    rows = []
                    for i in range(nx):
                        columns = []
                        for j in range(ny):
                            part = gr[step, (i * ny + j) * nz + k][:, None]
                            part = jnp.broadcast_to(part, (cx // per, per, cy, LANES)).reshape(cx, cy, LANES)
                            columns.append(jnp.where(own_group((cx, cy, LANES), width), part, 0.0))
                        rows.append(jnp.concatenate(columns, axis=1))
                    spot = lanes_dot(jnp.concatenate(rows, axis=0), gather_matrix(width, k * width))
                    fine = spot if fine is None else fine + spot
                chain = [fine]
                widths = [width * nz]
                for l in range(HALOED + 1, LEVELS):
                    widths.append(widths[-1] // 2)
                    chain.append(lanes_dot(fold_xy(chain[-1]), halve_matrix(widths[-1], 0)))
                whole = smooth_whole(chain[-1], widths[-1], LEVELS - 1)
                for l in range(LEVELS - 2, HALOED - 1, -1):
                    i = l - HALOED
                    spread_y(whole)
                    grown = spread[0:whole.shape[0], 0:2 * whole.shape[1], :]
                    grown = twice(lanes_dot(grown, double_matrix(widths[i + 1], 0)))
                    whole = grown + smooth_whole(chain[i], widths[i], l)
                wref[...] = whole
            receive(r, fields, HALOED)
            for l in range(HALOED):
                for x0, c in chunks(l):
                    mid, total = beside(r, fields[l], l, x0, c)
                    later[l][inside(l, x0, c)] = gref[l][x0:x0 + c] + (3.0 * mid + total) * (1.0 / 9.0)
        ends = [us[l][(SWEEPS - 1) % 2] for l in range(HALOED)]
        cx, cy, _ = dims[HALOED]
        spread_y(wref[pl.ds(at[0] * cx, cx)])
        part = spread[0:cx, pl.ds(pl.multiple_of(at[1] * 2 * cy, 8), 2 * cy), :]
        part = lanes_dot(part, double_matrix(width, at[2] * width))
        for l in range(HALOED - 1, -1, -1):
            X, Y, Z = dims[l]
            full = ends[l][1:X + 1, TOP:TOP + Y, :] * (4.0 ** l / 9.0) + twice(part)
            if l:
                spread_y(full)
                part = lanes_dot(spread[0:X, 0:2 * Y, :], double_matrix(Z, 0))
            else:
                ends[0][1:X + 1, TOP:TOP + Y, :] = full
        r = base + SWEEPS - 1
        z = ends[0]
        w = us[0][SWEEPS % 2]
        send(r, [z], 1)
        receive(r, [z], 1)
        rz = jnp.zeros((Y, LANES), jnp.float32)
        zw = jnp.zeros((Y, LANES), jnp.float32)
        for x0, c in chunks(0):
            mid, total = beside(r, z, 0, x0, c)
            image = 6.0 * mid - total
            w[inside(0, x0, c)] = image
            rz = rz + jnp.sum(g0[x0:x0 + c] * mid, axis=0)
            zw = zw + jnp.sum(mid * image, axis=0)
        sums = jnp.concatenate([jnp.sum(rz, axis=0, keepdims=True), jnp.sum(zw, axis=0, keepdims=True)], axis=0)
        ds[step] = sums
        dr[step, me] = sums
        to_all(step, ds, dr, dsend, drecv)
        all_done(step, dr, drecv)
        both = jnp.sum(dr[step], axis=0)
        both = jnp.sum(both, axis=1, keepdims=True)
        alpha = (both[0:1] / both[1:2])[None]
        for x0, c in chunks(0):
            sol_ref[x0:x0 + c] = sol_ref[x0:x0 + c] + alpha * z[inside(0, x0, c)]
            renewed = g0[x0:x0 + c] - alpha * w[inside(0, x0, c)]
            if step == STEPS - 1:
                res_ref[x0:x0 + c] = renewed
            else:
                g0[x0:x0 + c] = renewed

    for step in range(STEPS):
        all_done(step, gr, gsend)
        all_done(step, dr, dsend)
    for r in range(ROUNDS):
        for copy, cond, _ in halo_copies(r, 1 if r % SWEEPS == 0 else HALOED):
            pl.when(cond)(copy.wait_send)


def solution(mesh):
    sizes = tuple(mesh.shape[a] for a in AXES)
    n = sizes[0] * sizes[1] * sizes[2]

    def run(right_side, guess):
        X, Y, Z = block = guess.shape
        dims = [tuple(d >> l for d in block) for l in range(LEVELS)]
        rows = sum(dims[l][0] for l in range(HALOED))
        f32 = jnp.float32
        vm = lambda *s: pltpu.VMEM(s, f32)
        padded = [vm(dims[l][0] + 2, dims[l][1] + 2 * TOP, LANES) for l in range(HALOED) for _ in range(2)]
        cx, cy, width = dims[HALOED]
        packed = cx // plane_groups((cx, cy), width)
        scratch = padded + [vm(dims[l][0], dims[l][1], LANES) for l in range(HALOED)] + [
            vm(cx * sizes[0], cy * sizes[1], LANES),
            vm(X // 2, Y, LANES), vm(X // 2, Y, LANES),
            vm(ROUNDS, 2, rows, LANES), vm(ROUNDS, 2, rows, LANES),
            vm(ROUNDS, 2, rows, 1, LANES), vm(ROUNDS, 2, rows, 1, LANES),
            vm(ROUNDS, Y, LANES), vm(ROUNDS, 2, Y, LANES),
            vm(STEPS, packed, 1, LANES), vm(STEPS, n, packed, 1, LANES),
            vm(STEPS, 2, LANES), vm(STEPS, n, 2, LANES),
            pltpu.SemaphoreType.DMA((ROUNDS, 6)), pltpu.SemaphoreType.DMA((ROUNDS, 6)),
        ] + [pltpu.SemaphoreType.DMA((STEPS,))] * 4
        out = jax.ShapeDtypeStruct(block, f32)
        return tuple(pl.pallas_call(
            functools.partial(kernel, sizes, block),
            out_shape=(out, out),
            in_specs=[pl.BlockSpec(memory_space=pltpu.VMEM)] * 2,
            out_specs=[pl.BlockSpec(memory_space=pltpu.VMEM)] * 2,
            scratch_shapes=scratch,
            compiler_params=pltpu.CompilerParams(collective_id=0, has_side_effects=True),
        )(right_side, guess))

    spec = P(*AXES)
    return jax.shard_map(run, mesh=mesh, in_specs=(spec, spec), out_specs=(spec, spec), check_vma=False)
```

```python
import functools

import jax
import jax.numpy as jnp
from jax import lax
from jax.experimental import pallas as pl
from jax.experimental.pallas import tpu as pltpu
from jax.sharding import PartitionSpec as P

LEVELS = 6
SWEEPS = 4
STEPS = 2
HALOED = 3
AXES = ("gx", "gy", "gz")
LANES = 128
TOP = 8
MESH = pl.DeviceIdType.MESH
ROUNDS = 1 + STEPS * SWEEPS
HIGH = lax.Precision.HIGHEST


def iota(shape, dim):
    return lax.broadcasted_iota(jnp.int32, shape, dim)


def lanes_dot(x, matrix):
    first, second, _ = x.shape
    if second % 8 == 0:
        out = jnp.dot(x.reshape(first * second, LANES), matrix, precision=HIGH, preferred_element_type=jnp.float32)
        return out.reshape(first, second, LANES)
    planes = [jnp.dot(x[i], matrix, precision=HIGH, preferred_element_type=jnp.float32)[None] for i in range(first)]
    return jnp.concatenate(planes, axis=0)


def halve_matrix(width, start):
    source, target = iota((LANES, LANES), 0), iota((LANES, LANES), 1) - start
    keep = (target >= 0) & (target < width) & ((source == 2 * target) | (source == 2 * target + 1))
    return jnp.where(keep, 0.125, 0.0)


def double_matrix(width, start):
    source, target = iota((LANES, LANES), 0) - start, iota((LANES, LANES), 1)
    keep = (source >= 0) & (source < width) & ((target == 2 * source) | (target == 2 * source + 1))
    return jnp.where(keep, 1.0, 0.0)


def plane_groups(shape, width):
    return max(1, LANES // width // shape[1])


def own_group(shape, width):
    group = iota(shape, 0) % plane_groups(shape, width) * shape[1] + iota(shape, 1)
    return iota(shape, 2) // width == group


def tile_matrix(width):
    source, target = iota((LANES, LANES), 0), iota((LANES, LANES), 1) % width
    return jnp.where((source == 2 * target) | (source == 2 * target + 1), 0.125, 0.0)


def gather_matrix(width, start):
    source, target = iota((LANES, LANES), 0) % width, iota((LANES, LANES), 1) - start
    return jnp.where(source == target, 1.0, 0.0)


def kernel(sizes, block, b_ref, x_ref, sol_ref, res_ref, *rest):
    (u0a, u0b, u1a, u1b, u2a, u2b, g0, g1, g2, wref, fold, spread,
     xs, xr, ys, yr, zs, zr, gs, gr, ds, dr,
     hsend, hrecv, gsend, grecv, dsend, drecv) = rest
    us = ((u0a, u0b), (u1a, u1b), (u2a, u2b))
    gref = (g0, g1, g2)
    nx, ny, nz = sizes
    n = nx * ny * nz
    at = tuple(lax.axis_index(a) for a in AXES)
    me = (at[0] * ny + at[1]) * nz + at[2]
    dims = [tuple(d >> l for d in block) for l in range(LEVELS)]

    def others():
        moved = [[lax.rem(at[d] + k, sizes[d]) if k else at[d] for k in range(sizes[d])] for d in range(3)]
        return [(a, b, c) for a in moved[0] for b in moved[1] for c in moved[2]][1:]

    xr[...] = jnp.zeros_like(xr)
    yr[...] = jnp.zeros_like(yr)
    zr[...] = jnp.zeros_like(zr)

    barrier = pltpu.get_barrier_semaphore()

    for target in others():
        pl.semaphore_signal(barrier, inc=1, device_id=target, device_id_type=MESH)

    row_off, lane_off = [0], [0]
    for l in range(HALOED):
        row_off.append(row_off[-1] + dims[l][0])
        lane_off.append(lane_off[-1] + 2 * dims[l][0])

    def halo_copies(r, levels):
        rows = row_off[levels]
        out = []
        for d, (s, t) in enumerate(((xs, xr), (ys, yr), (zs, zr))):
            for side in (0, 1):
                target = list(at)
                target[d] = at[d] + (1 if side else -1)
                src = s.at[r] if d == 2 else s.at[r, side, pl.ds(0, rows)]
                dst = t.at[r, side] if d == 2 else t.at[r, side, pl.ds(0, rows)]
                copy = pltpu.make_async_remote_copy(
                    src_ref=src, dst_ref=dst,
                    send_sem=hsend.at[r, 2 * d + side], recv_sem=hrecv.at[r, 2 * d + side],
                    device_id=tuple(target), device_id_type=MESH,
                )
                lower, upper = at[d] > 0, at[d] < sizes[d] - 1
                out.append((copy, upper if side else lower, lower if side else upper))
        return out

    def send(r, fields, levels, before=lambda: None):
        for l in range(levels):
            X, Y, Z = dims[l]
            u = fields[l]
            o = row_off[l]
            for side, i in ((0, 1), (1, X)):
                xs[r, side, o:o + Y, :] = u[i, TOP:TOP + Y, :]
            for side, j in ((0, TOP), (1, TOP + Y - 1)):
                ys[r, side, o:o + X, :, :] = u[1:X + 1, j:j + 1, :]
            body = u[1:X + 1, TOP:TOP + Y, :]
            lane, plane = iota((X, Y, LANES), 2) - lane_off[l], iota((X, Y, LANES), 0)
            packed = jnp.where(lane == plane, body[:, :, Z - 1:Z], jnp.where(lane == plane + X, body[:, :, 0:1], 0.0))
            packed = jnp.sum(packed, axis=0)
            zs[r, 0:Y, :] = packed if l == 0 else zs[r, 0:Y, :] + packed
        before()
        for copy, cond, _ in halo_copies(r, levels):
            pl.when(cond)(copy.start)

    def receive(r, fields, levels):
        for copy, _, cond in halo_copies(r, levels):
            pl.when(cond)(copy.wait_recv)
        for l in range(levels):
            X, Y, Z = dims[l]
            u = fields[l]
            o = row_off[l]
            u[0, TOP:TOP + Y, :] = xr[r, 1, o:o + Y, :]
            u[X + 1, TOP:TOP + Y, :] = xr[r, 0, o:o + Y, :]
            u[1:X + 1, TOP - 1:TOP, :] = yr[r, 1, o:o + X, :, :]
            u[1:X + 1, TOP + Y:TOP + Y + 1, :] = yr[r, 0, o:o + X, :, :]

    def beside(r, u, l, x0, c):
        X, Y, Z = dims[l]
        mid = u[x0 + 1:x0 + 1 + c, TOP:TOP + Y, :]
        total = u[x0:x0 + c, TOP:TOP + Y, :] + u[x0 + 2:x0 + 2 + c, TOP:TOP + Y, :]
        total = total + u[x0 + 1:x0 + 1 + c, TOP - 1:TOP - 1 + Y, :]
        total = total + u[x0 + 1:x0 + 1 + c, TOP + 1:TOP + 1 + Y, :]
        lane = iota((c, Y, LANES), 2)
        o = lane_off[l] + x0
        low, high = zr[r, 1, 0:Y, :], zr[r, 0, 0:Y, :]
        below = jnp.concatenate([low[:, o + i:o + i + 1][None] for i in range(c)], axis=0)
        above = jnp.concatenate([high[:, o + X + i:o + X + i + 1][None] for i in range(c)], axis=0)
        total = total + jnp.where(lane == 0, below, pltpu.roll(mid, 1, 2))
        total = total + jnp.where(lane == Z - 1, above, pltpu.roll(mid, LANES - 1, 2))
        return mid, total

    def chunks(l):
        c = min(dims[l][0], 8)
        return [(x0, c) for x0 in range(0, dims[l][0], c)]

    def inside(l, x0, c):
        return (slice(x0 + 1, x0 + 1 + c), slice(TOP, TOP + dims[l][1]), slice(None))

    def fold_xy(field):
        X, Y, _ = field.shape
        pairs = field.reshape(X // 2, 2, Y, LANES)
        fold[0:X // 2, 0:Y, :] = pairs[:, 0] + pairs[:, 1]
        return fold[0:X // 2, pl.ds(0, Y // 2, 2), :] + fold[0:X // 2, pl.ds(1, Y // 2, 2), :]

    def spread_y(field):
        X, Y, _ = field.shape
        spread[0:X, pl.ds(0, Y, 2), :] = field
        spread[0:X, pl.ds(1, Y, 2), :] = field

    def twice(field):
        X, Y, _ = field.shape
        return jnp.broadcast_to(field[:, None], (X, 2, Y, LANES)).reshape(2 * X, Y, LANES)

    def to_all(step, src, dst, s_sem, r_sem):
        for target in others():
            pltpu.make_async_remote_copy(
                src_ref=src.at[step], dst_ref=dst.at[step, me], send_sem=s_sem.at[step], recv_sem=r_sem.at[step],
                device_id=target, device_id_type=MESH,
            ).start()

    def all_done(step, dst, sem):
        part = dst.at[step, pl.ds(0, n - 1)]
        pltpu.make_async_copy(part, part, sem.at[step]).wait()

    X, Y, Z = dims[0]
    u0a[1:X + 1, TOP:TOP + Y, :] = x_ref[...]
    sol_ref[...] = x_ref[...]
    send(0, [u0a], 1, lambda: pl.semaphore_wait(barrier, n - 1))
    receive(0, [u0a], 1)
    for x0, c in chunks(0):
        mid, total = beside(0, u0a, 0, x0, c)
        g0[x0:x0 + c] = b_ref[x0:x0 + c] - (6.0 * mid - total)

    def smooth_whole(rhs, width, l):
        X, Y, _ = rhs.shape
        lane = iota(rhs.shape, 2)
        e = rhs
        for _ in range(SWEEPS - 1):
            px, py = jnp.zeros((1, Y, LANES), jnp.float32), jnp.zeros((X, 1, LANES), jnp.float32)
            total = jnp.concatenate([px, e[:-1]], axis=0) + jnp.concatenate([e[1:], px], axis=0)
            total = total + jnp.concatenate([py, e[:, :-1]], axis=1) + jnp.concatenate([e[:, 1:], py], axis=1)
            total = total + jnp.where(lane == 0, 0.0, pltpu.roll(e, 1, 2))
            total = total + jnp.where(lane == width - 1, 0.0, pltpu.roll(e, LANES - 1, 2))
            e = rhs + (3.0 * e + total) * (1.0 / 9.0)
        return e * (4.0 ** l / 9.0)

    for step in range(STEPS):
        base = 1 + step * SWEEPS
        for l in range(HALOED - 1):
            gref[l + 1][...] = lanes_dot(fold_xy(gref[l][...]), halve_matrix(dims[l + 1][2], 0))
        width = dims[HALOED][2]
        own = lanes_dot(fold_xy(gref[HALOED - 1][...]), tile_matrix(width))
        own = jnp.where(own_group(own.shape, width), own, 0.0)
        own = jnp.sum(own.reshape(-1, plane_groups(own.shape, width), *own.shape[1:]), axis=1)
        own = jnp.sum(own, axis=1, keepdims=True)
        gs[step] = own
        gr[step, me] = own
        to_all(step, gs, gr, gsend, grecv)
        for l in range(HALOED):
            us[l][0][1:dims[l][0] + 1, TOP:TOP + dims[l][1], :] = gref[l][...]
        for sweep in range(SWEEPS - 1):
            r = base + sweep
            fields = [us[l][sweep % 2] for l in range(HALOED)]
            later = [us[l][(sweep + 1) % 2] for l in range(HALOED)]
            send(r, fields, HALOED)
            if sweep == SWEEPS - 2:
                all_done(step, gr, grecv)
                cx, cy, _ = dims[HALOED]
                per = plane_groups((cx, cy), width)
                fine = None
                for k in range(nz):
                    rows = []
                    for i in range(nx):
                        columns = []
                        for j in range(ny):
                            part = gr[step, (i * ny + j) * nz + k][:, None]
                            part = jnp.broadcast_to(part, (cx // per, per, cy, LANES)).reshape(cx, cy, LANES)
                            columns.append(jnp.where(own_group((cx, cy, LANES), width), part, 0.0))
                        rows.append(jnp.concatenate(columns, axis=1))
                    spot = lanes_dot(jnp.concatenate(rows, axis=0), gather_matrix(width, k * width))
                    fine = spot if fine is None else fine + spot
                chain = [fine]
                widths = [width * nz]
                for l in range(HALOED + 1, LEVELS):
                    widths.append(widths[-1] // 2)
                    chain.append(lanes_dot(fold_xy(chain[-1]), halve_matrix(widths[-1], 0)))
                whole = smooth_whole(chain[-1], widths[-1], LEVELS - 1)
                for l in range(LEVELS - 2, HALOED - 1, -1):
                    i = l - HALOED
                    spread_y(whole)
                    grown = spread[0:whole.shape[0], 0:2 * whole.shape[1], :]
                    grown = twice(lanes_dot(grown, double_matrix(widths[i + 1], 0)))
                    whole = grown + smooth_whole(chain[i], widths[i], l)
                wref[...] = whole
            receive(r, fields, HALOED)
            for l in range(HALOED):
                for x0, c in chunks(l):
                    mid, total = beside(r, fields[l], l, x0, c)
                    later[l][inside(l, x0, c)] = gref[l][x0:x0 + c] + (3.0 * mid + total) * (1.0 / 9.0)
        ends = [us[l][(SWEEPS - 1) % 2] for l in range(HALOED)]
        cx, cy, _ = dims[HALOED]
        spread_y(wref[pl.ds(at[0] * cx, cx)])
        part = spread[0:cx, pl.ds(pl.multiple_of(at[1] * 2 * cy, 8), 2 * cy), :]
        part = lanes_dot(part, double_matrix(width, at[2] * width))
        for l in range(HALOED - 1, -1, -1):
            X, Y, Z = dims[l]
            full = ends[l][1:X + 1, TOP:TOP + Y, :] * (4.0 ** l / 9.0) + twice(part)
            if l:
                spread_y(full)
                part = lanes_dot(spread[0:X, 0:2 * Y, :], double_matrix(Z, 0))
            else:
                ends[0][1:X + 1, TOP:TOP + Y, :] = full
        r = base + SWEEPS - 1
        z = ends[0]
        w = us[0][SWEEPS % 2]
        send(r, [z], 1)
        receive(r, [z], 1)
        rz = jnp.zeros((Y, LANES), jnp.float32)
        zw = jnp.zeros((Y, LANES), jnp.float32)
        for x0, c in chunks(0):
            mid, total = beside(r, z, 0, x0, c)
            image = 6.0 * mid - total
            w[inside(0, x0, c)] = image
            rz = rz + jnp.sum(g0[x0:x0 + c] * mid, axis=0)
            zw = zw + jnp.sum(mid * image, axis=0)
        sums = jnp.concatenate([jnp.sum(rz, axis=0, keepdims=True), jnp.sum(zw, axis=0, keepdims=True)], axis=0)
        ds[step] = sums
        dr[step, me] = sums
        to_all(step, ds, dr, dsend, drecv)
        all_done(step, dr, drecv)
        both = jnp.sum(dr[step], axis=0)
        both = jnp.sum(both, axis=1, keepdims=True)
        alpha = (both[0:1] / both[1:2])[None]
        for x0, c in chunks(0):
            sol_ref[x0:x0 + c] = sol_ref[x0:x0 + c] + alpha * z[inside(0, x0, c)]
            renewed = g0[x0:x0 + c] - alpha * w[inside(0, x0, c)]
            if step == STEPS - 1:
                res_ref[x0:x0 + c] = renewed
            else:
                g0[x0:x0 + c] = renewed

    for step in range(STEPS):
        all_done(step, gr, gsend)
        all_done(step, dr, dsend)
    for r in range(ROUNDS):
        for copy, cond, _ in halo_copies(r, 1 if r % SWEEPS == 0 else HALOED):
            pl.when(cond)(copy.wait_send)


def solution(mesh):
    sizes = tuple(mesh.shape[a] for a in AXES)
    n = sizes[0] * sizes[1] * sizes[2]

    def run(right_side, guess):
        X, Y, Z = block = guess.shape
        dims = [tuple(d >> l for d in block) for l in range(LEVELS)]
        rows = sum(dims[l][0] for l in range(HALOED))
        f32 = jnp.float32
        vm = lambda *s: pltpu.VMEM(s, f32)
        padded = [vm(dims[l][0] + 2, dims[l][1] + 2 * TOP, LANES) for l in range(HALOED) for _ in range(2)]
        cx, cy, width = dims[HALOED]
        packed = cx // plane_groups((cx, cy), width)
        scratch = padded + [vm(dims[l][0], dims[l][1], LANES) for l in range(HALOED)] + [
            vm(cx * sizes[0], cy * sizes[1], LANES),
            vm(X // 2, Y, LANES), vm(X // 2, Y, LANES),
            vm(ROUNDS, 2, rows, LANES), vm(ROUNDS, 2, rows, LANES),
            vm(ROUNDS, 2, rows, 1, LANES), vm(ROUNDS, 2, rows, 1, LANES),
            vm(ROUNDS, Y, LANES), vm(ROUNDS, 2, Y, LANES),
            vm(STEPS, packed, 1, LANES), vm(STEPS, n, packed, 1, LANES),
            vm(STEPS, 2, LANES), vm(STEPS, n, 2, LANES),
            pltpu.SemaphoreType.DMA((ROUNDS, 6)), pltpu.SemaphoreType.DMA((ROUNDS, 6)),
        ] + [pltpu.SemaphoreType.DMA((STEPS,))] * 4
        out = jax.ShapeDtypeStruct(block, f32)
        return tuple(pl.pallas_call(
            functools.partial(kernel, sizes, block),
            out_shape=(out, out),
            in_specs=[pl.BlockSpec(memory_space=pltpu.VMEM)] * 2,
            out_specs=[pl.BlockSpec(memory_space=pltpu.VMEM)] * 2,
            scratch_shapes=scratch,
            compiler_params=pltpu.CompilerParams(collective_id=0, has_side_effects=True),
        )(right_side, guess))

    spec = P(*AXES)
    return jax.shard_map(run, mesh=mesh, in_specs=(spec, spec), out_specs=(spec, spec), check_vma=False)
```
